32 devices in a mesh: grp: 8 (over z, y), row: 4 (over x, core).
Axes of the slice: x: 2, y: 2, z: 4, core: 2. Of those that a mesh axis runs over, the one named last changes fastest.
Arguments:
- block: bfloat16 [8192, 1024], P(('grp', 'row')), may hold values from -6 to 6
- degree: int32 [8192], P(('grp', 'row')), may hold values from 1 to 3
- tile_values: bfloat16 [2048, 128, 128], P(('grp', 'row')), may hold values from -0.1875 to 0.1875
- tile_rows: int32 [2048], P(('grp', 'row')), may hold values from 0 to 1
- tile_cols: int32 [2048], P(('grp', 'row')), may hold values from 0 to 15
- tile_count: int32 [32], P(('grp', 'row')), may hold values from 24 to 64, as said below
- send_tiles: int32 [32, 8], P(('grp', 'row')), may hold values from 0 to 1
Outputs:
- logs: bfloat16 [8192, 1024], P(('grp', 'row'))
- gram: float32 [8192, 1024], P(('grp', 'row'))
The draws below stay inside these ranges and needn't reach their ends.
Inputs may be any that keep to these rules, and one draw needn't show every extreme that they name: Slots of a device at positions tile_count or later are padding; some device has all 64 slots live.
All inputs are finite; a program needn't handle non-finite values.
Results may differ from the reference program's by a relative error of at most 0.014.
Values may be sent and summed in bfloat16 or wider, within the bound.
A program may use at most 128 MiB of HBM per device.

```python
import jax
import jax.numpy as jnp
from jax import lax

K = 1024
TILE = 128
ROWS_DEV = 256
SLOTS = 64
POWERS = 2
ROW_TILES = 2
NODES = 8192
SOURCES = 16
SLOTS_ALL = 2048
N_GRP = 8
N_ROW = 4


def draw_tile_count(key, part):
    first_key, second_key = jax.random.split(jax.random.fold_in(key, 7))
    devices = N_GRP * N_ROW
    drawn = jax.random.randint(first_key, (devices,), 0, SLOTS + 1)
    counts = jnp.minimum(SLOTS * 3 // 8 + drawn * drawn * 5 // (8 * SLOTS), SLOTS)
    chosen = jax.random.randint(second_key, (), 0, devices)
    counts = jnp.where(jnp.arange(devices) == chosen, SLOTS, counts)
    return counts.astype(jnp.int32)


def with_ends(values, stream_key, least, top_value):
    spot = [jax.random.randint(jax.random.fold_in(stream_key, axis), (), 0, length) for axis, length in enumerate(values.shape)]
    longest = values.shape.index(max(values.shape))
    beside = spot[:longest] + [(spot[longest] + 1) % values.shape[longest]] + spot[longest + 1:]
    return values.at[tuple(spot)].set(least).at[tuple(beside)].set(top_value)


def steps_of(key, extent, cuts, low, largest):
    gain, own = 1.0, jax.random.fold_in(key, 6)
    for axis_at, blocks in cuts:
        heights = jnp.exp(jax.random.uniform(jax.random.fold_in(own, axis_at), (blocks,), jnp.float32, low / len(cuts), largest / len(cuts)))
        gain = gain * jnp.repeat(heights, extent[axis_at] // blocks).reshape([-1 if axis == axis_at else 1 for axis in range(len(extent))])
    return gain


def centred(stream_key, extent, spread, reach, cuts=(), kind=jnp.bfloat16):
    gain = steps_of(stream_key, extent, cuts, -0.22, 0.18) if cuts else 1.0
    values = jax.random.normal(stream_key, extent, jnp.float32) * spread * gain
    return jnp.minimum(jnp.maximum(values, -reach), reach).astype(kind)


def setup_inputs(seed: int = 0) -> dict:
    key_of = jax.random.split(jax.random.key(seed), 8)
    return {
        "block": centred(key_of[0], (NODES, K), 1.0, 6.0, ((0, 32),)),
        "degree": with_ends(jax.random.randint(key_of[1], (NODES,), 1, 4), jax.random.fold_in(key_of[1], 1), 1, 3).astype(jnp.int32),
        "tile_values": centred(key_of[2], (SLOTS_ALL, TILE, TILE), (SLOTS * 16) ** -0.5, 0.1875, ((0, 32),)),
        "tile_rows": with_ends(jax.random.randint(key_of[3], (SLOTS_ALL,), 0, ROW_TILES), jax.random.fold_in(key_of[3], 1), 0, ROW_TILES - 1).astype(jnp.int32),
        "tile_cols": with_ends(jax.random.randint(key_of[4], (SLOTS_ALL,), 0, SOURCES), jax.random.fold_in(key_of[4], 1), 0, SOURCES - 1).astype(jnp.int32),
        "tile_count": draw_tile_count(jax.random.fold_in(key_of[7], 71), 0),
        "send_tiles": with_ends(jax.random.randint(key_of[6], (N_GRP * N_ROW, N_GRP), 0, ROW_TILES), jax.random.fold_in(key_of[6], 1), 0, ROW_TILES - 1).astype(jnp.int32),
    }


def column_tiles(tile_cols, send_tiles):
    row_tiles = ROWS_DEV // TILE
    slot_ids = jnp.arange(SLOTS * N_GRP * N_ROW, dtype=jnp.int32)
    device = slot_ids // SLOTS
    group = device // N_ROW
    member = device % N_ROW
    local_span = N_ROW * row_tiles
    source_group = jnp.maximum(tile_cols - local_span, 0)
    source_device = (source_group * N_ROW + member).astype(jnp.int32)
    remote = source_device * row_tiles + send_tiles[source_device, group]
    return jnp.where(tile_cols < local_span, group * local_span + tile_cols, remote).astype(jnp.int32)


def reference(block, degree, tile_values, tile_rows, tile_cols, tile_count, send_tiles):
    devices = N_GRP * N_ROW
    row_tiles = ROWS_DEV // TILE
    columns = column_tiles(tile_cols, send_tiles).reshape(devices, SLOTS)
    values = tile_values.reshape(devices, SLOTS, TILE, TILE)
    rows = tile_rows.reshape(devices, SLOTS)
    tile_ids = jnp.arange(row_tiles, dtype=jnp.int32)
    slot_pos = jnp.arange(SLOTS, dtype=jnp.int32)
    current = block
    power_sum = jnp.zeros(block.shape, jnp.float32)
    for power in range(POWERS):
        tiles_all = current.reshape(-1, TILE, K).astype(jnp.float32)

        def one_device(pieces):
            values_here, columns_here, rows_here, count_here = pieces
            picked = tiles_all[columns_here]
            products = jnp.einsum("sik,skf->sif", values_here.astype(jnp.float32), picked, precision=lax.Precision.HIGHEST)
            live_mask = slot_pos < count_here
            weights = ((rows_here[None, :] == tile_ids[:, None]) & live_mask[None, :]).astype(jnp.float32)
            return jnp.einsum("rs,sif->rif", weights, products, precision=lax.Precision.HIGHEST)

        summed = lax.map(one_device, (values, columns, rows, tile_count))
        current = (summed.reshape(-1, K) / degree[:, None].astype(jnp.float32)).astype(jnp.bfloat16)
        power_sum = power_sum + current.astype(jnp.float32)
    logs = jnp.log(jnp.maximum(3.0 * power_sum, 1.0)).astype(jnp.bfloat16)
    grouped = logs.reshape(N_GRP, N_ROW * ROWS_DEV, K)

    def group_gram(group_logs):
        return jnp.dot(group_logs.T, group_logs, preferred_element_type=jnp.float32)

    gram = lax.map(group_gram, grouped) / (N_ROW * ROWS_DEV)
    return logs, gram.reshape(N_GRP * K, K)
```

```python
import functools

import jax
import jax.numpy as jnp
from jax import lax
from jax.experimental import pallas as pl
from jax.experimental.pallas import tpu as pltpu
from jax.sharding import PartitionSpec as P

POWERS = 2
MESH = pl.DeviceIdType.MESH


def matrix_kernel(sources, rows_ref, cols_ref, count_ref, degree_ref, values_ref, out_ref, sums):
    tile = values_ref.shape[1]
    row_tiles = out_ref.shape[0] // tile

    def clear(index, carry):
        sums[index] = jnp.zeros(sums.shape[1:], jnp.float32)
        return carry

    lax.fori_loop(0, row_tiles * sources, clear, 0)

    def add_slot(slot, carry):
        place = rows_ref[slot] * sources + cols_ref[slot]
        sums[place] += values_ref[slot].astype(jnp.float32)
        return carry

    lax.fori_loop(0, count_ref[0], add_slot, 0)
    for row in range(row_tiles):
        degree = degree_ref[row : row + 1, :].astype(jnp.float32)
        scale = (1.0 / jnp.broadcast_to(degree, (tile, tile))).T
        for col in range(sources):
            part = sums[row * sources + col] * scale
            out_ref[row * tile : (row + 1) * tile, col * tile : (col + 1) * tile] = part.astype(jnp.bfloat16)


def step_kernel(
    groups, ranks, send_ref, matrix_ref, block_ref, logs_ref, gram_ref,
    source, own, staged, total, everyone, mine,
    grp_send, grp_recv, row_send, row_recv, pass_send,
):
    chunks, _, row_tiles, tile, width = own.shape
    local = ranks * row_tiles
    g = lax.axis_index("grp")
    r = lax.axis_index("row")
    core = lax.rem(r, 2)
    partner = r + 1 - 2 * core
    pairs = ranks // 2

    def other_group(step):
        return lax.rem(g + step, groups)

    def same_core(step):
        return lax.rem(r + 2 * step, ranks)

    barrier = pltpu.get_barrier_semaphore()
    for step in range(1, groups):
        pl.semaphore_signal(barrier, inc=1, device_id=(other_group(step), r), device_id_type=MESH)
    for step in range(1, ranks):
        pl.semaphore_signal(barrier, inc=1, device_id=(g, lax.rem(r + step, ranks)), device_id_type=MESH)

    def land(phase, j, rank):
        where = pl.ds(rank * row_tiles, row_tiles)
        return source.at[phase, j, where] if phase < POWERS else everyone.at[j, where]

    def row_copy(phase, j, to):
        origin = own.at[j, phase]
        return pltpu.make_async_remote_copy(
            src_ref=origin, dst_ref=land(phase, j, r),
            send_sem=row_send.at[phase, j, to], recv_sem=row_recv.at[phase, j, r],
            device_id=(g, to), device_id_type=MESH)

    def pass_copy(phase, j, rank):
        spot = land(phase, j, rank)
        return pltpu.make_async_remote_copy(
            src_ref=spot, dst_ref=spot,
            send_sem=pass_send.at[phase, j, rank], recv_sem=row_recv.at[phase, j, rank],
            device_id=(g, partner), device_id_type=MESH)

    def row_arrival(phase, j, rank):
        spot = land(phase, j, rank)
        return pltpu.make_async_remote_copy(
            src_ref=spot, dst_ref=spot,
            send_sem=pass_send.at[phase, j, rank], recv_sem=row_recv.at[phase, j, rank],
            device_id=(g, partner), device_id_type=MESH)

    def grp_copy(phase, j, to):
        return pltpu.make_async_remote_copy(
            src_ref=staged.at[phase, j, to], dst_ref=source.at[phase, j, local + g],
            send_sem=grp_send.at[phase, j, to], recv_sem=grp_recv.at[phase, j, g],
            device_id=(to, r), device_id_type=MESH)

    def grp_arrival(phase, j, group):
        return pltpu.make_async_remote_copy(
            src_ref=staged.at[phase, j, group], dst_ref=source.at[phase, j, local + group],
            send_sem=grp_send.at[phase, j, group], recv_sem=grp_recv.at[phase, j, group],
            device_id=(group, r), device_id_type=MESH)

    def stage(phase, j):
        for step in range(1, groups):
            to = other_group(step)
            staged[phase, j, to] = own[j, phase, send_ref[0, to]]
        source[phase, j, local + g] = own[j, phase, send_ref[0, g]]

    def keep(phase, j, value):
        tiles = value.reshape(row_tiles, tile, width)
        own[j, phase] = tiles
        if phase < POWERS:
            source[phase, j, pl.ds(r * row_tiles, row_tiles)] = tiles
        else:
            everyone[j, pl.ds(r * row_tiles, row_tiles)] = tiles

    def send(phase, j):
        if phase < POWERS:
            for step in range(1, groups):
                grp_copy(phase, j, other_group(step)).start()
        for step in range(1, pairs):
            row_copy(phase, j, same_core(step)).start()
        row_copy(phase, j, partner).start()

    def receive(phase, j):
        for step in range(1, pairs):
            rank = lax.rem(r + ranks - 2 * step, ranks)
            row_arrival(phase, j, rank).wait_recv()
            pass_copy(phase, j, rank).start()
        row_arrival(phase, j, partner).wait_recv()
        for step in range(1, pairs):
            row_arrival(phase, j, lax.rem(partner + ranks - 2 * step, ranks)).wait_recv()
        if phase < POWERS:
            for step in range(1, groups):
                grp_arrival(phase, j, lax.rem(g + groups - step, groups)).wait_recv()

    for j in range(chunks):
        keep(0, j, block_ref[:, j * width : (j + 1) * width])
        stage(0, j)
    pl.semaphore_wait(barrier, groups + ranks - 2)
    for j in range(chunks):
        send(0, j)
    for phase in range(POWERS):
        for j in range(chunks):
            receive(phase, j)
            summed = jnp.dot(
                matrix_ref[...], source[phase, j].reshape(-1, width),
                preferred_element_type=jnp.float32)
            current = summed.astype(jnp.bfloat16)
            if phase == 0:
                total[j] = current.astype(jnp.float32)
            else:
                total[j] += current.astype(jnp.float32)
            if phase < POWERS - 1:
                keep(phase + 1, j, current)
                stage(phase + 1, j)
            else:
                logs = jnp.log(jnp.maximum(3.0 * total[j], 1.0)).astype(jnp.bfloat16)
                logs_ref[:, j * width : (j + 1) * width] = logs
                keep(phase + 1, j, logs)
            send(phase + 1, j)
    for j in range(chunks):
        receive(POWERS, j)
    mine[...] = everyone[r].reshape(-1, width).T
    rows_all = row_tiles * tile * ranks
    for j in range(chunks):
        part = jnp.dot(mine[...], everyone[j].reshape(-1, width), preferred_element_type=jnp.float32)
        gram_ref[:, j * width : (j + 1) * width] = part / rows_all
    for phase in range(POWERS + 1):
        for j in range(chunks):
            if phase < POWERS:
                for step in range(1, groups):
                    grp_copy(phase, j, other_group(step)).wait_send()
            for step in range(1, pairs):
                row_copy(phase, j, same_core(step)).wait_send()
                pass_copy(phase, j, lax.rem(r + ranks - 2 * step, ranks)).wait_send()
            row_copy(phase, j, partner).wait_send()


def body(block, degree, tile_values, tile_rows, tile_cols, tile_count, send_tiles):
    rows_here, width = block.shape
    tile = tile_values.shape[1]
    row_tiles = rows_here // tile
    ranks = lax.axis_size("row")
    groups = lax.axis_size("grp")
    sources = ranks * row_tiles + groups
    smem = pl.BlockSpec(memory_space=pltpu.SMEM)
    vmem = pl.BlockSpec(memory_space=pltpu.VMEM)
    matrix = pl.pallas_call(
        functools.partial(matrix_kernel, sources),
        out_shape=jax.ShapeDtypeStruct((rows_here, sources * tile), jnp.bfloat16),
        in_specs=[smem, smem, smem, vmem, vmem],
        out_specs=vmem,
        scratch_shapes=[pltpu.VMEM((row_tiles * sources, tile, tile), jnp.float32)],
        name="matrix",
    )(tile_rows, tile_cols, tile_count, degree.reshape(row_tiles, tile), tile_values)
    share = width // ranks
    chunks = ranks
    dma = pltpu.SemaphoreType.DMA
    logs, gram = pl.pallas_call(
        functools.partial(step_kernel, groups, ranks),
        out_shape=(
            jax.ShapeDtypeStruct((rows_here, width), jnp.bfloat16),
            jax.ShapeDtypeStruct((share, width), jnp.float32),
        ),
        in_specs=[smem, vmem, vmem],
        out_specs=(vmem, vmem),
        scratch_shapes=[
            pltpu.VMEM((POWERS, chunks, sources, tile, share), jnp.bfloat16),
            pltpu.VMEM((chunks, POWERS + 1, row_tiles, tile, share), jnp.bfloat16),
            pltpu.VMEM((POWERS, chunks, groups, tile, share), jnp.bfloat16),
            pltpu.VMEM((chunks, rows_here, share), jnp.float32),
            pltpu.VMEM((chunks, ranks * row_tiles, tile, share), jnp.bfloat16),
            pltpu.VMEM((share, rows_here * ranks), jnp.bfloat16),
            dma((POWERS, chunks, groups)),
            dma((POWERS, chunks, groups)),
            dma((POWERS + 1, chunks, ranks)),
            dma((POWERS + 1, chunks, ranks)),
            dma((POWERS + 1, chunks, ranks)),
        ],
        compiler_params=pltpu.CompilerParams(
            collective_id=0, has_side_effects=True, vmem_limit_bytes=60 * 1024 * 1024),
        name="step",
    )(send_tiles, matrix, block)
    return logs, gram


def solution(mesh):
    placed = (
        P(("grp", "row"), None),
        P(("grp", "row")),
        P(("grp", "row"), None, None),
        P(("grp", "row")),
        P(("grp", "row")),
        P(("grp", "row")),
        P(("grp", "row"), None),
    )
    return jax.shard_map(
        body,
        mesh=mesh,
        in_specs=placed,
        out_specs=(P(("grp", "row"), None), P(("grp", "row"), None)),
        check_vma=False,
    )
```

```python
import functools

import jax
import jax.numpy as jnp
from jax import lax
from jax.experimental import pallas as pl
from jax.experimental.pallas import tpu as pltpu
from jax.sharding import PartitionSpec as P

POWERS = 2
MESH = pl.DeviceIdType.MESH


def order_kernel(sources, rows_ref, cols_ref, count_ref, before_ref, last_ref):
    slots = rows_ref.shape[0]

    def clear(place, carry):
        last_ref[place] = slots
        return carry

    def skip(slot, carry):
        before_ref[slot] = slots
        return carry

    def link(slot, carry):
        place = rows_ref[slot] * sources + cols_ref[slot]
        before_ref[slot] = last_ref[place]
        last_ref[place] = slot
        return carry

    lax.fori_loop(0, last_ref.shape[0], clear, 0)
    lax.fori_loop(0, slots, skip, 0)
    lax.fori_loop(0, count_ref[0], link, 0)


def step_kernel(
    groups, ranks, send_ref, before_ref, last_ref, degree_ref, values_hbm, block_ref, logs_ref, gram_ref,
    values_ref, sums, matrix_ref, values_sem, source, own, staged, total, everyone, mine,
    grp_send, grp_recv, row_send, row_recv, pass_send,
):
    chunks, _, row_tiles, tile, width = own.shape
    local = ranks * row_tiles
    g = lax.axis_index("grp")
    r = lax.axis_index("row")
    core = lax.rem(r, 2)
    partner = r + 1 - 2 * core
    pairs = ranks // 2

    slots = values_ref.shape[0]
    sources = source.shape[2]
    load = pltpu.make_async_copy(values_hbm, values_ref, values_sem)
    load.start()

    def other_group(step):
        return lax.rem(g + step, groups)

    def same_core(step):
        return lax.rem(r + 2 * step, ranks)

    barrier = pltpu.get_barrier_semaphore()
    for step in range(1, groups):
        pl.semaphore_signal(barrier, inc=1, device_id=(other_group(step), r), device_id_type=MESH)
    for step in range(1, ranks):
        pl.semaphore_signal(barrier, inc=1, device_id=(g, lax.rem(r + step, ranks)), device_id_type=MESH)

    def land(phase, j, rank):
        where = pl.ds(rank * row_tiles, row_tiles)
        return source.at[phase, j, where] if phase < POWERS else everyone.at[j, where]

    def row_copy(phase, j, to):
        origin = own.at[j, phase]
        return pltpu.make_async_remote_copy(
            src_ref=origin, dst_ref=land(phase, j, r),
            send_sem=row_send.at[phase, j, to], recv_sem=row_recv.at[phase, j, r],
            device_id=(g, to), device_id_type=MESH)

    def pass_copy(phase, j, rank):
        spot = land(phase, j, rank)
        return pltpu.make_async_remote_copy(
            src_ref=spot, dst_ref=spot,
            send_sem=pass_send.at[phase, j, rank], recv_sem=row_recv.at[phase, j, rank],
            device_id=(g, partner), device_id_type=MESH)

    def row_arrival(phase, j, rank):
        spot = land(phase, j, rank)
        return pltpu.make_async_remote_copy(
            src_ref=spot, dst_ref=spot,
            send_sem=pass_send.at[phase, j, rank], recv_sem=row_recv.at[phase, j, rank],
            device_id=(g, partner), device_id_type=MESH)

    def grp_copy(phase, j, to):
        return pltpu.make_async_remote_copy(
            src_ref=staged.at[phase, j, to], dst_ref=source.at[phase, j, local + g],
            send_sem=grp_send.at[phase, j, to], recv_sem=grp_recv.at[phase, j, g],
            device_id=(to, r), device_id_type=MESH)

    def grp_arrival(phase, j, group):
        return pltpu.make_async_remote_copy(
            src_ref=staged.at[phase, j, group], dst_ref=source.at[phase, j, local + group],
            send_sem=grp_send.at[phase, j, group], recv_sem=grp_recv.at[phase, j, group],
            device_id=(group, r), device_id_type=MESH)

    def stage(phase, j):
        for step in range(1, groups):
            to = other_group(step)
            staged[phase, j, to] = own[j, phase, send_ref[0, to]]
        source[phase, j, local + g] = own[j, phase, send_ref[0, g]]

    def keep(phase, j, value):
        tiles = value.reshape(row_tiles, tile, width)
        own[j, phase] = tiles
        if phase < POWERS:
            source[phase, j, pl.ds(r * row_tiles, row_tiles)] = tiles
        else:
            everyone[j, pl.ds(r * row_tiles, row_tiles)] = tiles

    def send(phase, j):
        if phase < POWERS:
            for step in range(1, groups):
                grp_copy(phase, j, other_group(step)).start()
        for step in range(1, pairs):
            row_copy(phase, j, same_core(step)).start()
        row_copy(phase, j, partner).start()

    def receive(phase, j):
        for step in range(1, pairs):
            rank = lax.rem(r + ranks - 2 * step, ranks)
            row_arrival(phase, j, rank).wait_recv()
            pass_copy(phase, j, rank).start()
        row_arrival(phase, j, partner).wait_recv()
        for step in range(1, pairs):
            row_arrival(phase, j, lax.rem(partner + ranks - 2 * step, ranks)).wait_recv()
        if phase < POWERS:
            for step in range(1, groups):
                grp_arrival(phase, j, lax.rem(g + groups - step, groups)).wait_recv()

    for j in range(chunks):
        keep(0, j, block_ref[:, j * width : (j + 1) * width])
        stage(0, j)
    pl.semaphore_wait(barrier, groups + ranks - 2)
    for j in range(chunks):
        send(0, j)
    def clear(slot, carry):
        sums[slot] = jnp.zeros(sums.shape[1:], jnp.float32)
        return carry

    def add_slot(slot, carry):
        sums[slot] = sums[before_ref[slot]] + values_ref[slot].astype(jnp.float32)
        return carry

    lax.fori_loop(0, slots + 1, clear, 0)
    load.wait()
    lax.fori_loop(0, slots, add_slot, 0)
    for row in range(row_tiles):
        degree = degree_ref[row : row + 1, :].astype(jnp.float32)
        scale = (1.0 / jnp.broadcast_to(degree, (tile, tile))).T
        for col in range(sources):
            part = sums[last_ref[row * sources + col]] * scale
            matrix_ref[row * tile : (row + 1) * tile, col * tile : (col + 1) * tile] = part.astype(jnp.bfloat16)
    for phase in range(POWERS):
        for j in range(chunks):
            receive(phase, j)
            summed = jnp.dot(
                matrix_ref[...], source[phase, j].reshape(-1, width),
                preferred_element_type=jnp.float32)
            current = summed.astype(jnp.bfloat16)
            if phase == 0:
                total[j] = current.astype(jnp.float32)
            else:
                total[j] += current.astype(jnp.float32)
            if phase < POWERS - 1:
                keep(phase + 1, j, current)
                stage(phase + 1, j)
            else:
                logs = jnp.log(jnp.maximum(3.0 * total[j], 1.0)).astype(jnp.bfloat16)
                logs_ref[:, j * width : (j + 1) * width] = logs
                keep(phase + 1, j, logs)
            send(phase + 1, j)
    for j in range(chunks):
        receive(POWERS, j)
    mine[...] = everyone[r].reshape(-1, width).T
    rows_all = row_tiles * tile * ranks
    for j in range(chunks):
        part = jnp.dot(mine[...], everyone[j].reshape(-1, width), preferred_element_type=jnp.float32)
        gram_ref[:, j * width : (j + 1) * width] = part / rows_all
    for phase in range(POWERS + 1):
        for j in range(chunks):
            if phase < POWERS:
                for step in range(1, groups):
                    grp_copy(phase, j, other_group(step)).wait_send()
            for step in range(1, pairs):
                row_copy(phase, j, same_core(step)).wait_send()
                pass_copy(phase, j, lax.rem(r + ranks - 2 * step, ranks)).wait_send()
            row_copy(phase, j, partner).wait_send()


def body(block, degree, tile_values, tile_rows, tile_cols, tile_count, send_tiles):
    rows_here, width = block.shape
    tile = tile_values.shape[1]
    row_tiles = rows_here // tile
    ranks = lax.axis_size("row")
    groups = lax.axis_size("grp")
    sources = ranks * row_tiles + groups
    smem = pl.BlockSpec(memory_space=pltpu.SMEM)
    vmem = pl.BlockSpec(memory_space=pltpu.VMEM)
    slots = tile_values.shape[0]
    before, last = pl.pallas_call(
        functools.partial(order_kernel, sources),
        out_shape=(
            jax.ShapeDtypeStruct((slots,), jnp.int32),
            jax.ShapeDtypeStruct((row_tiles * sources,), jnp.int32),
        ),
        in_specs=[smem, smem, smem],
        out_specs=(smem, smem),
        name="order",
    )(tile_rows, tile_cols, tile_count)
    share = width // ranks
    chunks = ranks
    dma = pltpu.SemaphoreType.DMA
    logs, gram = pl.pallas_call(
        functools.partial(step_kernel, groups, ranks),
        out_shape=(
            jax.ShapeDtypeStruct((rows_here, width), jnp.bfloat16),
            jax.ShapeDtypeStruct((share, width), jnp.float32),
        ),
        in_specs=[smem, smem, smem, vmem, pl.BlockSpec(memory_space=pl.ANY), vmem],
        out_specs=(vmem, vmem),
        scratch_shapes=[
            pltpu.VMEM(tile_values.shape, jnp.bfloat16),
            pltpu.VMEM((slots + 1, tile, tile), jnp.float32),
            pltpu.VMEM((rows_here, sources * tile), jnp.bfloat16),
            dma,
            pltpu.VMEM((POWERS, chunks, sources, tile, share), jnp.bfloat16),
            pltpu.VMEM((chunks, POWERS + 1, row_tiles, tile, share), jnp.bfloat16),
            pltpu.VMEM((POWERS, chunks, groups, tile, share), jnp.bfloat16),
            pltpu.VMEM((chunks, rows_here, share), jnp.float32),
            pltpu.VMEM((chunks, ranks * row_tiles, tile, share), jnp.bfloat16),
            pltpu.VMEM((share, rows_here * ranks), jnp.bfloat16),
            dma((POWERS, chunks, groups)),
            dma((POWERS, chunks, groups)),
            dma((POWERS + 1, chunks, ranks)),
            dma((POWERS + 1, chunks, ranks)),
            dma((POWERS + 1, chunks, ranks)),
        ],
        compiler_params=pltpu.CompilerParams(
            collective_id=0, has_side_effects=True, vmem_limit_bytes=60 * 1024 * 1024),
        name="step",
    )(send_tiles, before, last, degree.reshape(row_tiles, tile), tile_values, block)
    return logs, gram


def solution(mesh):
    placed = (
        P(("grp", "row"), None),
        P(("grp", "row")),
        P(("grp", "row"), None, None),
        P(("grp", "row")),
        P(("grp", "row")),
        P(("grp", "row")),
        P(("grp", "row"), None),
    )
    return jax.shard_map(
        body,
        mesh=mesh,
        in_specs=placed,
        out_specs=(P(("grp", "row"), None), P(("grp", "row"), None)),
        check_vma=False,
    )
```

```python
import functools

import jax
import jax.numpy as jnp
from jax import lax
from jax.experimental import pallas as pl
from jax.experimental.pallas import tpu as pltpu
from jax.sharding import PartitionSpec as P

POWERS = 2
MESH = pl.DeviceIdType.MESH


def order_kernel(sources, rows_ref, cols_ref, count_ref, before_ref, last_ref):
    slots = rows_ref.shape[0]

    def clear(place, carry):
        last_ref[place] = slots
        return carry

    def skip(slot, carry):
        before_ref[slot] = slots
        return carry

    def link(slot, carry):
        place = rows_ref[slot] * sources + cols_ref[slot]
        before_ref[slot] = last_ref[place]
        last_ref[place] = slot
        return carry

    lax.fori_loop(0, last_ref.shape[0], clear, 0)
    lax.fori_loop(0, slots, skip, 0)
    lax.fori_loop(0, count_ref[0], link, 0)


def step_kernel(
    groups, ranks, send_ref, before_ref, last_ref, degree_ref, values_hbm, block_ref, logs_ref, gram_ref,
    values_ref, sums, matrix_ref, values_sem, source, own, staged, total, everyone, mine,
    grp_send, grp_recv, row_send, row_recv, pass_send,
):
    chunks, _, row_tiles, tile, width = own.shape
    local = ranks * row_tiles
    g = lax.axis_index("grp")
    r = lax.axis_index("row")
    core = lax.rem(r, 2)
    partner = r + 1 - 2 * core
    pairs = ranks // 2

    slots = values_ref.shape[0]
    sources = source.shape[2]
    load = pltpu.make_async_copy(values_hbm, values_ref, values_sem)
    load.start()

    def other_group(step):
        return lax.rem(g + step, groups)

    def same_core(step):
        return lax.rem(r + 2 * step, ranks)

    barrier = pltpu.get_barrier_semaphore()
    for step in range(1, groups):
        pl.semaphore_signal(barrier, inc=1, device_id=(other_group(step), r), device_id_type=MESH)
    for step in range(1, ranks):
        pl.semaphore_signal(barrier, inc=1, device_id=(g, lax.rem(r + step, ranks)), device_id_type=MESH)

    def land(phase, j, rank):
        where = pl.ds(rank * row_tiles, row_tiles)
        return source.at[phase, j, where] if phase < POWERS else everyone.at[j, where]

    def row_copy(phase, j, to):
        origin = own.at[j, phase]
        return pltpu.make_async_remote_copy(
            src_ref=origin, dst_ref=land(phase, j, r),
            send_sem=row_send.at[phase, j, to], recv_sem=row_recv.at[phase, j, r],
            device_id=(g, to), device_id_type=MESH)

    def pass_copy(phase, j, rank):
        spot = land(phase, j, rank)
        return pltpu.make_async_remote_copy(
            src_ref=spot, dst_ref=spot,
            send_sem=pass_send.at[phase, j, rank], recv_sem=row_recv.at[phase, j, rank],
            device_id=(g, partner), device_id_type=MESH)

    def row_arrival(phase, j, rank):
        spot = land(phase, j, rank)
        return pltpu.make_async_remote_copy(
            src_ref=spot, dst_ref=spot,
            send_sem=pass_send.at[phase, j, rank], recv_sem=row_recv.at[phase, j, rank],
            device_id=(g, partner), device_id_type=MESH)

    def grp_copy(phase, j, to):
        return pltpu.make_async_remote_copy(
            src_ref=staged.at[phase, j, to], dst_ref=source.at[phase, j, local + g],
            send_sem=grp_send.at[phase, j, to], recv_sem=grp_recv.at[phase, j, g],
            device_id=(to, r), device_id_type=MESH)

    def grp_arrival(phase, j, group):
        return pltpu.make_async_remote_copy(
            src_ref=staged.at[phase, j, group], dst_ref=source.at[phase, j, local + group],
            send_sem=grp_send.at[phase, j, group], recv_sem=grp_recv.at[phase, j, group],
            device_id=(group, r), device_id_type=MESH)

    def stage(phase, j):
        for step in range(1, groups):
            to = other_group(step)
            staged[phase, j, to] = own[j, phase, send_ref[0, to]]
        source[phase, j, local + g] = own[j, phase, send_ref[0, g]]

    def keep(phase, j, value):
        tiles = value.reshape(row_tiles, tile, width)
        own[j, phase] = tiles
        if phase < POWERS:
            source[phase, j, pl.ds(r * row_tiles, row_tiles)] = tiles
        else:
            everyone[j, pl.ds(r * row_tiles, row_tiles)] = tiles

    def send(phase, j):
        if phase < POWERS:
            for step in sorted(range(1, groups), key=lambda step: abs(2 * step - groups)):
                grp_copy(phase, j, other_group(step)).start()
        for step in range(1, pairs):
            row_copy(phase, j, same_core(step)).start()
        row_copy(phase, j, partner).start()

    def receive(phase, j):
        for step in range(1, pairs):
            rank = lax.rem(r + ranks - 2 * step, ranks)
            row_arrival(phase, j, rank).wait_recv()
            pass_copy(phase, j, rank).start()
        row_arrival(phase, j, partner).wait_recv()
        for step in range(1, pairs):
            row_arrival(phase, j, lax.rem(partner + ranks - 2 * step, ranks)).wait_recv()
        if phase < POWERS:
            for step in range(1, groups):
                grp_arrival(phase, j, lax.rem(g + groups - step, groups)).wait_recv()

    for j in range(chunks):
        keep(0, j, block_ref[:, j * width : (j + 1) * width])
        stage(0, j)
    pl.semaphore_wait(barrier, groups + ranks - 2)
    for j in range(chunks):
        send(0, j)
    def clear(slot, carry):
        sums[slot] = jnp.zeros(sums.shape[1:], jnp.float32)
        return carry

    def add_slot(slot, carry):
        sums[slot] = sums[before_ref[slot]] + values_ref[slot].astype(jnp.float32)
        return carry

    lax.fori_loop(0, slots + 1, clear, 0)
    load.wait()
    lax.fori_loop(0, slots, add_slot, 0)
    for row in range(row_tiles):
        degree = degree_ref[row : row + 1, :].astype(jnp.float32)
        scale = (1.0 / jnp.broadcast_to(degree, (tile, tile))).T
        for col in range(sources):
            part = sums[last_ref[row * sources + col]] * scale
            matrix_ref[row * tile : (row + 1) * tile, col * tile : (col + 1) * tile] = part.astype(jnp.bfloat16)
    for phase in range(POWERS):
        for j in range(chunks):
            receive(phase, j)
            summed = jnp.dot(
                matrix_ref[...], source[phase, j].reshape(-1, width),
                preferred_element_type=jnp.float32)
            current = summed.astype(jnp.bfloat16)
            if phase == 0:
                total[j] = current.astype(jnp.float32)
            else:
                total[j] += current.astype(jnp.float32)
            if phase < POWERS - 1:
                keep(phase + 1, j, current)
                stage(phase + 1, j)
            else:
                logs = jnp.log(jnp.maximum(3.0 * total[j], 1.0)).astype(jnp.bfloat16)
                logs_ref[:, j * width : (j + 1) * width] = logs
                keep(phase + 1, j, logs)
            send(phase + 1, j)
    for j in range(chunks):
        receive(POWERS, j)
    mine[...] = everyone[r].reshape(-1, width).T
    rows_all = row_tiles * tile * ranks
    for j in range(chunks):
        part = jnp.dot(mine[...], everyone[j].reshape(-1, width), preferred_element_type=jnp.float32)
        gram_ref[:, j * width : (j + 1) * width] = part / rows_all
    for phase in range(POWERS + 1):
        for j in range(chunks):
            if phase < POWERS:
                for step in range(1, groups):
                    grp_copy(phase, j, other_group(step)).wait_send()
            for step in range(1, pairs):
                row_copy(phase, j, same_core(step)).wait_send()
                pass_copy(phase, j, lax.rem(r + ranks - 2 * step, ranks)).wait_send()
            row_copy(phase, j, partner).wait_send()


def body(block, degree, tile_values, tile_rows, tile_cols, tile_count, send_tiles):
    rows_here, width = block.shape
    tile = tile_values.shape[1]
    row_tiles = rows_here // tile
    ranks = lax.axis_size("row")
    groups = lax.axis_size("grp")
    sources = ranks * row_tiles + groups
    smem = pl.BlockSpec(memory_space=pltpu.SMEM)
    vmem = pl.BlockSpec(memory_space=pltpu.VMEM)
    slots = tile_values.shape[0]
    before, last = pl.pallas_call(
        functools.partial(order_kernel, sources),
        out_shape=(
            jax.ShapeDtypeStruct((slots,), jnp.int32),
            jax.ShapeDtypeStruct((row_tiles * sources,), jnp.int32),
        ),
        in_specs=[smem, smem, smem],
        out_specs=(smem, smem),
        name="order",
    )(tile_rows, tile_cols, tile_count)
    share = width // ranks
    chunks = ranks
    dma = pltpu.SemaphoreType.DMA
    logs, gram = pl.pallas_call(
        functools.partial(step_kernel, groups, ranks),
        out_shape=(
            jax.ShapeDtypeStruct((rows_here, width), jnp.bfloat16),
            jax.ShapeDtypeStruct((share, width), jnp.float32),
        ),
        in_specs=[smem, smem, smem, vmem, pl.BlockSpec(memory_space=pl.ANY), vmem],
        out_specs=(vmem, vmem),
        scratch_shapes=[
            pltpu.VMEM(tile_values.shape, jnp.bfloat16),
            pltpu.VMEM((slots + 1, tile, tile), jnp.float32),
            pltpu.VMEM((rows_here, sources * tile), jnp.bfloat16),
            dma,
            pltpu.VMEM((POWERS, chunks, sources, tile, share), jnp.bfloat16),
            pltpu.VMEM((chunks, POWERS + 1, row_tiles, tile, share), jnp.bfloat16),
            pltpu.VMEM((POWERS, chunks, groups, tile, share), jnp.bfloat16),
            pltpu.VMEM((chunks, rows_here, share), jnp.float32),
            pltpu.VMEM((chunks, ranks * row_tiles, tile, share), jnp.bfloat16),
            pltpu.VMEM((share, rows_here * ranks), jnp.bfloat16),
            dma((POWERS, chunks, groups)),
            dma((POWERS, chunks, groups)),
            dma((POWERS + 1, chunks, ranks)),
            dma((POWERS + 1, chunks, ranks)),
            dma((POWERS + 1, chunks, ranks)),
        ],
        compiler_params=pltpu.CompilerParams(
            collective_id=0, has_side_effects=True, vmem_limit_bytes=60 * 1024 * 1024),
        name="step",
    )(send_tiles, before, last, degree.reshape(row_tiles, tile), tile_values, block)
    return logs, gram


def solution(mesh):
    placed = (
        P(("grp", "row"), None),
        P(("grp", "row")),
        P(("grp", "row"), None, None),
        P(("grp", "row")),
        P(("grp", "row")),
        P(("grp", "row")),
        P(("grp", "row"), None),
    )
    return jax.shard_map(
        body,
        mesh=mesh,
        in_specs=placed,
        out_specs=(P(("grp", "row"), None), P(("grp", "row"), None)),
        check_vma=False,
    )
```
